32 devices in a mesh: sky: 4 (over x, core), tm: 8 (over z, y).
Axes of the slice: x: 2, y: 2, z: 4, core: 2. Of those that a mesh axis runs over, the one named last changes fastest.
Arguments:
- attitude: float32 [4, 8, 512], P(None, 'tm', 'sky'), may hold values from -6 to 6
- slot_time: float32 [262144], P(('sky', 'tm')), may hold values from -1 to 1
- slot_parallax: float32 [262144], P(('sky', 'tm')), may hold values from -1 to 1
- slot_observed: float32 [262144], P(('sky', 'tm')), may hold values from -6 to 6
- slot_phase: float32 [262144], P(('sky', 'tm')), may hold values from 0 to 1
- slot_knot: int32 [262144], P(('sky', 'tm')), may hold values from 0 to 508
- block_source: int32 [8192], P(('sky', 'tm')), may hold values from 0 to 63
- block_count: int32 [8192], P(('sky', 'tm')), may hold values from 1 to 32
- prior: float32 [5, 256], P(None, ('sky', 'tm')), may hold values from 0.5 to 4
Outputs:
- update: float32 [5, 256], P(None, ('sky', 'tm'))
The draws below stay inside these ranges and needn't reach their ends.
Inputs may be any that keep to these rules, and one draw needn't show every extreme that they name: The four knots from slot_knot on lie in the transit's time group of 512 knots. `block_source`: an index into the 64 sources of the block's own sky sector.
All inputs are finite; a program needn't handle non-finite values.
Results may differ from the reference program's by a relative error of at most 0.0003.
Values sent between devices are 32-bit elements; how exact they have to be, the bound alone decides.
A program may use at most 64 MiB of HBM per device.

```python
import math
import jax
import jax.numpy as jnp
from jax import lax

SLOTS = 32
PARAMS = 5
SRC_SKY = 64
SOURCES = 256
KNOTS_GROUP = 512
BLOCKS = 8192
TRANSITS = 262144
N_SKY = 4
N_TM = 8


def plant(values, key, low, high):
    longest = values.shape.index(max(values.shape))
    spots = []
    for shift in (0, 1):
        where = [jax.random.randint(jax.random.fold_in(key, axis), (), 0, length) for axis, length in enumerate(values.shape)]
        where[longest] = (where[longest] + shift) % values.shape[longest]
        spots.append(tuple(where))
    return values.at[spots[0]].set(low).at[spots[1]].set(high)


def shard_levels(stream_key, extent, cuts, low, top_value):
    loudness, own = 1.0, jax.random.fold_in(stream_key, 6)
    for dim, shards_of in cuts:
        heights = jnp.exp(jax.random.uniform(jax.random.fold_in(own, dim), (shards_of,), jnp.float32, low / len(cuts), top_value / len(cuts)))
        loudness = loudness * jnp.repeat(heights, extent[dim] // shards_of).reshape([-1 if axis == dim else 1 for axis in range(len(extent))])
    return loudness


def centred(key, shape, deviation, reach, shards=(), kind=jnp.bfloat16):
    values = deviation * jax.random.normal(key, shape, jnp.float32)
    if shards:
        values = values * shard_levels(key, shape, shards, -0.22, 0.18)
    return jnp.clip(values, -reach, reach).astype(kind)


def setup_inputs(seed: int = 0) -> dict:
    key_list = jax.random.split(jax.random.key(seed), 10)
    return {
        "attitude": centred(key_list[0], (4, N_TM, KNOTS_GROUP), 1.0, 6.0, ((1, 8), (2, 4)), jnp.float32),
        "slot_time": jnp.clip(jax.random.uniform(key_list[1], (TRANSITS,), jnp.float32, -1.0, 1.0) * shard_levels(key_list[1], (TRANSITS,), ((0, 32),), -0.4, 0.0), -1.0, 1.0),
        "slot_parallax": jnp.clip(jax.random.uniform(key_list[2], (TRANSITS,), jnp.float32, -1.0, 1.0) * shard_levels(key_list[2], (TRANSITS,), ((0, 32),), -0.4, 0.0), -1.0, 1.0),
        "slot_observed": centred(key_list[3], (TRANSITS,), 1.0, 6.0, ((0, 32),), jnp.float32),
        "slot_phase": jnp.clip(1.0 * jax.random.uniform(key_list[4], (TRANSITS,), jnp.float32) ** shard_levels(key_list[4], (TRANSITS,), ((0, 32),), -0.2, 0.2), 0.0, 1.0),
        "slot_knot": plant(jax.random.randint(key_list[5], (TRANSITS,), 0, KNOTS_GROUP - 3), jax.random.fold_in(key_list[5], 1), 0, (KNOTS_GROUP - 3) - 1).astype(jnp.int32),
        "block_source": plant(jax.random.randint(key_list[6], (BLOCKS,), 0, SRC_SKY), jax.random.fold_in(key_list[6], 1), 0, SRC_SKY - 1).astype(jnp.int32),
        "block_count": plant(jax.random.randint(key_list[7], (BLOCKS,), 1, SLOTS + 1), jax.random.fold_in(key_list[7], 1), 1, SLOTS).astype(jnp.int32),
        "prior": jnp.clip(jnp.exp(math.log(4.0) - 2.0794415 * jax.random.uniform(key_list[8], (PARAMS, SOURCES), jnp.float32) ** shard_levels(key_list[8], (PARAMS, SOURCES), ((1, 32),), -0.2, 0.2)), 0.5, 4.0),
    }


PAIR_LIST = [(i, j) for i in range(5) for j in range(i, 5)]

def block_sums(table, knot, phase, time, parallax, observed, count):
    weights = [(1.0 - phase) ** 3 / 6.0, (3.0 * phase ** 3 - 6.0 * phase ** 2 + 4.0) / 6.0, (-3.0 * phase ** 3 + 3.0 * phase ** 2 + 3.0 * phase + 1.0) / 6.0, phase ** 3 / 6.0]
    quat = weights[0][None, :] * table[:, knot]
    for i in range(1, 4):
        quat = quat + weights[i][None, :] * table[:, knot + i]
    cross = quat[0] * quat[0] + quat[1] * quat[1] - quat[2] * quat[2] - quat[3] * quat[3]
    along = 2.0 * (quat[1] * quat[2] + quat[0] * quat[3])
    tilt = 2.0 * (quat[1] * quat[3] - quat[0] * quat[2])
    design = [cross, along, parallax, time * cross, time * along]
    residual = observed - tilt
    rows = [design[i] * design[j] for i, j in PAIR_LIST] + [design[i] * residual for i in range(5)]
    stacked = jnp.stack(rows)
    blocks = count.shape[0]
    stacked = stacked.reshape(20, blocks, -1)
    live = (jnp.arange(stacked.shape[2], dtype=jnp.int32)[None, :] < count[:, None]).astype(stacked.dtype)
    return lax.optimization_barrier(jnp.sum(stacked * live[None], axis=2))

def solve_normals(normal, prior):
    entry = {}
    for index, pair in enumerate(PAIR_LIST):
        entry[pair[1], pair[0]] = normal[index]
    for i in range(5):
        entry[i, i] = entry[i, i] + prior[i]
    lower = {}
    for col in range(5):
        pivot = entry[col, col]
        for k in range(col):
            pivot = pivot - lower[col, k] * lower[col, k]
        root = jnp.sqrt(pivot)
        lower[col, col] = root
        for row in range(col + 1, 5):
            value = entry[row, col]
            for k in range(col):
                value = value - lower[row, k] * lower[col, k]
            lower[row, col] = value / root
    forward = []
    for i in range(5):
        value = normal[15 + i]
        for k in range(i):
            value = value - lower[i, k] * forward[k]
        forward.append(value / lower[i, i])
    result = [None] * 5
    for i in range(4, -1, -1):
        value = forward[i]
        for k in range(i + 1, 5):
            value = value - lower[k, i] * result[k]
        result[i] = value / lower[i, i]
    return jnp.stack(result)

def reference(attitude, slot_time, slot_parallax, slot_observed, slot_phase, slot_knot, block_source, block_count, prior):

    def per_slot(array):
        return array.reshape(N_SKY, N_TM, -1)
    prior_sky = jnp.transpose(prior.reshape(5, N_SKY, SRC_SKY), (1, 0, 2))

    def sector(items):
        knot, phase, time, parallax, observed, source, count, prior_here = items
        sums = jax.vmap(block_sums, in_axes=(1, 0, 0, 0, 0, 0, 0))(attitude, knot, phase, time, parallax, observed, count)
        flat = jnp.transpose(sums, (1, 0, 2)).reshape(20, -1)
        normal = jnp.zeros((20, SRC_SKY), jnp.float32).at[:, source.reshape(-1)].add(flat)
        return solve_normals(normal, prior_here)
    solved = lax.map(sector, (per_slot(slot_knot), per_slot(slot_phase), per_slot(slot_time), per_slot(slot_parallax), per_slot(slot_observed), per_slot(block_source), per_slot(block_count), prior_sky))
    return jnp.transpose(solved, (1, 0, 2)).reshape(5, SOURCES)
```

```python
import functools

import jax
import jax.numpy as jnp
from jax import lax
from jax.experimental import pallas as pl
from jax.experimental.pallas import tpu as pltpu
from jax.sharding import PartitionSpec as P

PAIR_LIST = [(i, j) for i in range(5) for j in range(i, 5)]
MESH = pl.DeviceIdType.MESH
LANES = 128
ROWS = 32


def lane_gather(row, index):
    wide = jnp.broadcast_to(row, index.shape)
    return jnp.take_along_axis(wide, index, axis=1, mode="promise_in_bounds")


def split3(value):
    high = value.astype(jnp.bfloat16)
    rest = value - high.astype(jnp.float32)
    mid = rest.astype(jnp.bfloat16)
    low = (rest - mid.astype(jnp.float32)).astype(jnp.bfloat16)
    return high, mid, low


def solve_rows(row, prior_row):
    entry = {}
    for index, (i, j) in enumerate(PAIR_LIST):
        entry[j, i] = row(index)
    for i in range(5):
        entry[i, i] = entry[i, i] + prior_row(i)
    right = [row(15 + i) for i in range(5)]
    unit, inverse = {}, []
    for col in range(5):
        inv = 1.0 / entry[col, col]
        inverse.append(inv)
        for r in range(col + 1, 5):
            unit[r, col] = entry[r, col] * inv
        for r in range(col + 1, 5):
            for c in range(col + 1, r + 1):
                entry[r, c] = entry[r, c] - unit[r, col] * entry[c, col]
            right[r] = right[r] - unit[r, col] * right[col]
    result = [right[i] * inverse[i] for i in range(5)]
    for i in range(4, 0, -1):
        for k in range(i):
            result[k] = result[k] - unit[i, k] * result[i]
    return result


def kernel(
    n_sky, n_tm, span,
    attitude_hbm, time_hbm, parallax_hbm, observed_hbm, phase_hbm, knot_hbm,
    source_hbm, count_hbm, prior_hbm,
    out_ref,
    table, coef, time_v, parallax_v, observed_v, phase_v, knot_v, source_v, count_v, prior_v,
    spread, parts, member, tiles, landed, turned,
    local_sem, own_sem, att_send, att_recv, sum_send, sum_recv,
):
    sky = lax.axis_index("sky")
    tm = lax.axis_index("tm")
    rows = time_v.shape[0]
    owned = prior_v.shape[1]
    sources = owned * n_tm
    segs = LANES // span

    barrier = pltpu.get_barrier_semaphore()
    for d in range(1, n_sky):
        pl.semaphore_signal(
            barrier, inc=1, device_id={"sky": lax.rem(sky + d, n_sky)}, device_id_type=MESH
        )
    for d in range(1, n_tm):
        pl.semaphore_signal(
            barrier, inc=1, device_id={"tm": lax.rem(tm + d, n_tm)}, device_id_type=MESH
        )
    own = pltpu.make_async_copy(attitude_hbm, table.at[sky], own_sem)
    own.start()
    locals_ = []
    pairs = (
        (count_hbm, count_v), (source_hbm, source_v), (knot_hbm, knot_v), (phase_hbm, phase_v),
        (time_hbm, time_v), (parallax_hbm, parallax_v), (observed_hbm, observed_v),
        (prior_hbm, prior_v),
    )
    for i, (src, dst) in enumerate(pairs):
        copy = pltpu.make_async_copy(src, dst, local_sem.at[i])
        copy.start()
        locals_.append(copy)

    lane_out = lax.broadcasted_iota(jnp.int32, (LANES, LANES), 1)
    lane_in = lax.broadcasted_iota(jnp.int32, (LANES, LANES), 0)
    base = lane_out - (lane_in // span) * ROWS
    for x in range(20):
        spread[x * LANES : (x + 1) * LANES, :] = jnp.where(base == x, 1.0, 0.0).astype(jnp.bfloat16)

    pl.semaphore_wait(barrier, n_sky - 1 + n_tm - 1)

    sends = []
    for d in range(1, n_sky):
        copy = pltpu.make_async_remote_copy(
            src_ref=attitude_hbm,
            dst_ref=table.at[sky],
            send_sem=att_send.at[d - 1],
            recv_sem=att_recv.at[d - 1],
            device_id={"sky": lax.rem(sky + d, n_sky)},
            device_id_type=MESH,
        )
        copy.start()
        sends.append(copy)

    for copy in locals_:
        copy.wait()

    width = 3 * rows
    lane = lax.broadcasted_iota(jnp.int32, (8, LANES), 1)
    sub = lax.broadcasted_iota(jnp.int32, (8, LANES), 0)
    id_list = []
    for start in range(0, width, LANES):
        block = ((lane + start) % rows) * segs + sub % segs
        got = lane_gather(source_v[0:1, :], block % LANES)
        for c in range(1, source_v.shape[0]):
            got = jnp.where(block // LANES == c, lane_gather(source_v[c : c + 1, :], block % LANES), got)
        id_list.append(got)
    ids = jnp.concatenate(id_list, axis=1)[:, :width]
    which = lax.broadcasted_iota(jnp.int32, (sources, width), 0)
    for q in range(segs):
        hit = jnp.broadcast_to(ids[q : q + 1, :], (sources, width)) == which
        member[q * sources : (q + 1) * sources, :] = jnp.where(hit, 1.0, 0.0).astype(jnp.bfloat16)

    own.wait()
    for d in range(1, n_sky):
        pltpu.make_async_remote_copy(
            src_ref=attitude_hbm,
            dst_ref=table.at[lax.rem(sky + n_sky - d, n_sky)],
            send_sem=att_send.at[d - 1],
            recv_sem=att_recv.at[d - 1],
            device_id={"sky": lax.rem(sky + d, n_sky)},
            device_id_type=MESH,
        ).wait_recv()

    per = table.shape[2] // LANES
    chunks = [
        table[c // per, :, (c % per) * LANES : (c % per + 1) * LANES] for c in range(n_sky * per)
    ]
    n_chunks = len(chunks)
    here = jnp.concatenate(chunks, axis=0)
    after = jnp.concatenate(chunks[1:] + chunks[-1:], axis=0)
    wide_lane = lax.broadcasted_iota(jnp.int32, here.shape, 1)
    a = [here]
    for i in range(1, 4):
        a.append(
            jnp.where(
                wide_lane < LANES - i,
                pltpu.roll(here, LANES - i, 1),
                pltpu.roll(after, LANES - i, 1),
            )
        )
    coef[0] = (a[0] + 4.0 * a[1] + a[2]) * (1.0 / 6.0)
    coef[1] = (a[2] - a[0]) * 0.5
    coef[2] = (a[0] - 2.0 * a[1] + a[2]) * 0.5
    coef[3] = ((a[3] - a[0]) + 3.0 * (a[1] - a[2])) * (1.0 / 6.0)

    def sums_of(v):
        at = slice(v * 8, v * 8 + 8)
        knot = knot_v[at, :]
        u = phase_v[at, :]
        time = time_v[at, :]
        block = (sub + v * 8) * segs + lane // span
        chunk = (v * 8 * segs) // LANES
        count = lane_gather(count_v[chunk : chunk + 1, :], block - chunk * LANES)
        live = lane % span < count
        low, high = knot % LANES, knot // LANES
        picks = [high == c for c in range(n_chunks)]
        quat = []
        for m in range(4):
            value = None
            for j in (3, 2, 1, 0):
                got = lane_gather(coef[j, m : m + 1, :], low)
                for c in range(1, n_chunks):
                    x = c * 4 + m
                    got = jnp.where(picks[c], lane_gather(coef[j, x : x + 1, :], low), got)
                value = got if value is None else value * u + got
            quat.append(value)
        q0, q1, q2, q3 = quat
        cross = jnp.where(live, q0 * q0 + q1 * q1 - q2 * q2 - q3 * q3, 0.0)
        along = jnp.where(live, 2.0 * (q1 * q2 + q0 * q3), 0.0)
        tilt = 2.0 * (q1 * q3 - q0 * q2)
        parallax = jnp.where(live, parallax_v[at, :], 0.0)
        design = [cross, along, parallax, time * cross, time * along]
        residual = observed_v[at, :] - tilt
        return [design[i] * design[j] for i, j in PAIR_LIST] + [d * residual for d in design]

    for v in range(0, rows // 8, 2):
        first, second = sums_of(v), sums_of(v + 1)
        for x in range(20):
            for k, part in enumerate(split3(jnp.concatenate([first[x], second[x]], axis=0))):
                parts[k * rows + v * 8 : k * rows + v * 8 + 16, x * LANES : (x + 1) * LANES] = part

    three = jnp.dot(parts[...], spread[...], preferred_element_type=jnp.float32)
    block_sum = three[:rows] + three[rows : 2 * rows] + three[2 * rows :]
    stacked = jnp.concatenate(split3(block_sum), axis=0)
    by_seg = jnp.dot(member[...], stacked, preferred_element_type=jnp.float32)
    lane_s = lax.broadcasted_iota(jnp.int32, (sources, LANES), 1) // ROWS
    normal = jnp.where(lane_s == 0, by_seg[:sources], 0.0)
    for q in range(1, segs):
        normal = jnp.where(lane_s == q, by_seg[q * sources : (q + 1) * sources], normal)
    tiles[...] = normal.reshape(n_tm, owned, LANES)

    for d in range(1, n_tm):
        peer = lax.rem(tm + d, n_tm)
        copy = pltpu.make_async_remote_copy(
            src_ref=tiles.at[peer],
            dst_ref=landed.at[d - 1],
            send_sem=sum_send.at[d - 1],
            recv_sem=sum_recv.at[d - 1],
            device_id={"tm": peer},
            device_id_type=MESH,
        )
        copy.start()
        sends.append(copy)
    total = tiles[tm]
    for copy in sends[n_sky - 1 :]:
        copy.wait_recv()
    for d in range(1, n_tm):
        total = total + landed[d - 1]
    for shift in range(1, segs):
        pass
    full = total
    for q in range(1, segs):
        full = full + pltpu.roll(total, q * ROWS, 1)
    turned[...] = jnp.transpose(full)
    result = solve_rows(lambda i: turned[i : i + 1, :], lambda i: prior_v[i : i + 1, :])
    for i in range(5):
        out_ref[i : i + 1, :] = result[i]
    for copy in sends:
        copy.wait_send()


def on_device(n_sky, n_tm, attitude, time, parallax, observed, phase, knot, source, count, prior):
    slots, blocks, owned = time.shape[0], source.shape[0], prior.shape[1]
    knots = attitude.shape[2]
    rows = slots // LANES
    span = slots // blocks
    sources = owned * n_tm
    segs = LANES // span
    n_chunks = n_sky * knots // LANES
    shape = (rows, LANES)
    vmem = pltpu.VMEM
    f32, i32, bf16 = jnp.float32, jnp.int32, jnp.bfloat16
    return pl.pallas_call(
        functools.partial(kernel, n_sky, n_tm, span),
        out_shape=jax.ShapeDtypeStruct(prior.shape, f32),
        in_specs=[pl.BlockSpec(memory_space=pl.ANY)] * 9,
        out_specs=pl.BlockSpec(memory_space=pltpu.VMEM),
        scratch_shapes=[
            vmem((n_sky, 4, knots), f32),
            vmem((4, n_chunks * 4, LANES), f32),
            vmem(shape, f32),
            vmem(shape, f32),
            vmem(shape, f32),
            vmem(shape, f32),
            vmem(shape, i32),
            vmem((blocks // LANES, LANES), i32),
            vmem((blocks // LANES, LANES), i32),
            vmem(prior.shape, f32),
            vmem((20 * LANES, LANES), bf16),
            vmem((3 * rows, 20 * LANES), bf16),
            vmem((segs * sources, 3 * rows), bf16),
            vmem((n_tm, owned, LANES), f32),
            vmem((n_tm - 1, owned, LANES), f32),
            vmem((LANES, owned), f32),
            pltpu.SemaphoreType.DMA((8,)),
            pltpu.SemaphoreType.DMA,
            pltpu.SemaphoreType.DMA((n_sky - 1,)),
            pltpu.SemaphoreType.DMA((n_sky - 1,)),
            pltpu.SemaphoreType.DMA((n_tm - 1,)),
            pltpu.SemaphoreType.DMA((n_tm - 1,)),
        ],
        compiler_params=pltpu.CompilerParams(collective_id=0, has_side_effects=True),
    )(
        attitude.reshape(4, knots),
        time.reshape(shape),
        parallax.reshape(shape),
        observed.reshape(shape),
        phase.reshape(shape),
        knot.reshape(shape),
        source.reshape(blocks // LANES, LANES),
        count.reshape(blocks // LANES, LANES),
        prior,
    )


def solution(mesh):
    slot = P(("sky", "tm"))
    in_specs = (P(None, "tm", "sky"),) + (slot,) * 7 + (P(None, ("sky", "tm")),)
    return jax.shard_map(
        functools.partial(on_device, mesh.shape["sky"], mesh.shape["tm"]),
        mesh=mesh,
        in_specs=in_specs,
        out_specs=P(None, ("sky", "tm")),
        check_vma=False,
    )
```

```python
import functools

import jax
import jax.numpy as jnp
from jax import lax
from jax.experimental import pallas as pl
from jax.experimental.pallas import tpu as pltpu
from jax.sharding import PartitionSpec as P

PAIR_LIST = [(i, j) for i in range(5) for j in range(i, 5)]
MESH = pl.DeviceIdType.MESH
LANES = 128
ROWS = 32


def lane_gather(row, index):
    wide = jnp.broadcast_to(row, index.shape)
    return jnp.take_along_axis(wide, index, axis=1, mode="promise_in_bounds")


def split3(value):
    high = value.astype(jnp.bfloat16)
    rest = value - high.astype(jnp.float32)
    mid = rest.astype(jnp.bfloat16)
    low = (rest - mid.astype(jnp.float32)).astype(jnp.bfloat16)
    return high, mid, low


def solve_rows(row, prior_row):
    entry = {}
    for index, (i, j) in enumerate(PAIR_LIST):
        entry[j, i] = row(index)
    for i in range(5):
        entry[i, i] = entry[i, i] + prior_row(i)
    right = [row(15 + i) for i in range(5)]
    unit, inverse = {}, []
    for col in range(5):
        inv = 1.0 / entry[col, col]
        inverse.append(inv)
        for r in range(col + 1, 5):
            unit[r, col] = entry[r, col] * inv
        for r in range(col + 1, 5):
            for c in range(col + 1, r + 1):
                entry[r, c] = entry[r, c] - unit[r, col] * entry[c, col]
            right[r] = right[r] - unit[r, col] * right[col]
    result = [right[i] * inverse[i] for i in range(5)]
    for i in range(4, 0, -1):
        for k in range(i):
            result[k] = result[k] - unit[i, k] * result[i]
    return result


def kernel(
    n_sky, n_tm, span,
    attitude_hbm, time_hbm, parallax_hbm, observed_hbm, phase_hbm, knot_hbm,
    source_hbm, count_hbm,
    out_ref,
    table, coef, reals, ints, spread, parts, member, tiles, landed,
    real_sem, int_sem, att_send, att_recv, sum_send, sum_recv,
):
    sky = lax.axis_index("sky")
    tm = lax.axis_index("tm")
    rows = time_hbm.shape[0]
    owned = tiles.shape[1]
    wide = source_hbm.shape[0]
    phase_v, time_v, parallax_v, observed_v = (reals.at[i] for i in range(4))
    knot_v = ints.at[:rows]
    source_v = ints.at[rows : rows + wide]
    count_v = ints.at[rows + wide :]
    sources = owned * n_tm
    segs = LANES // span

    barrier = pltpu.get_barrier_semaphore()
    for d in range(1, n_sky):
        pl.semaphore_signal(
            barrier, inc=1, device_id={"sky": lax.rem(sky + d, n_sky)}, device_id_type=MESH
        )
    for d in range(1, n_tm):
        pl.semaphore_signal(
            barrier, inc=1, device_id={"tm": lax.rem(tm + d, n_tm)}, device_id_type=MESH
        )
    pltpu.make_async_copy(attitude_hbm, table.at[sky], att_recv).start()
    for src, dst in ((source_hbm, source_v), (count_hbm, count_v), (knot_hbm, knot_v)):
        pltpu.make_async_copy(src, dst, int_sem).start()
    for i, src in enumerate((phase_hbm, time_hbm, parallax_hbm, observed_hbm)):
        pltpu.make_async_copy(src, reals.at[i], real_sem).start()

    lane_out = lax.broadcasted_iota(jnp.int32, (LANES, LANES), 1)
    lane_in = lax.broadcasted_iota(jnp.int32, (LANES, LANES), 0)
    base = lane_out - (lane_in // span) * ROWS
    for x in range(20):
        spread[x * LANES : (x + 1) * LANES, :] = jnp.where(base == x, 1.0, 0.0).astype(jnp.bfloat16)

    pl.semaphore_wait(barrier, n_sky - 1 + n_tm - 1)

    for d in range(1, n_sky):
        pltpu.make_async_remote_copy(
            src_ref=attitude_hbm,
            dst_ref=table.at[sky],
            send_sem=att_send,
            recv_sem=att_recv,
            device_id={"sky": lax.rem(sky + d, n_sky)},
            device_id_type=MESH,
        ).start()

    pltpu.make_async_copy(ints, ints, int_sem).wait()

    width = 3 * rows
    lane = lax.broadcasted_iota(jnp.int32, (8, LANES), 1)
    sub = lax.broadcasted_iota(jnp.int32, (8, LANES), 0)
    id_list = []
    for start in range(0, width, LANES):
        block = ((lane + start) % rows) * segs + sub % segs
        got = lane_gather(source_v[0:1, :], block % LANES)
        for c in range(1, source_v.shape[0]):
            got = jnp.where(block // LANES == c, lane_gather(source_v[c : c + 1, :], block % LANES), got)
        id_list.append(got)
    ids = jnp.concatenate(id_list, axis=1)[:, :width]
    which = lax.broadcasted_iota(jnp.int32, (sources, width), 0)
    for q in range(segs):
        hit = jnp.broadcast_to(ids[q : q + 1, :], (sources, width)) == which
        member[q * sources : (q + 1) * sources, :] = jnp.where(hit, 1.0, 0.0).astype(jnp.bfloat16)

    pltpu.make_async_copy(reals, reals, real_sem).wait()
    pltpu.make_async_copy(table, table, att_recv).wait()

    per = table.shape[2] // LANES
    chunks = [
        table[c // per, :, (c % per) * LANES : (c % per + 1) * LANES] for c in range(n_sky * per)
    ]
    n_chunks = len(chunks)
    here = jnp.concatenate(chunks, axis=0)
    after = jnp.concatenate(chunks[1:] + chunks[-1:], axis=0)
    wide_lane = lax.broadcasted_iota(jnp.int32, here.shape, 1)
    a = [here]
    for i in range(1, 4):
        a.append(
            jnp.where(
                wide_lane < LANES - i,
                pltpu.roll(here, LANES - i, 1),
                pltpu.roll(after, LANES - i, 1),
            )
        )
    coef[0] = (a[0] + 4.0 * a[1] + a[2]) * (1.0 / 6.0)
    coef[1] = (a[2] - a[0]) * 0.5
    coef[2] = (a[0] - 2.0 * a[1] + a[2]) * 0.5
    coef[3] = ((a[3] - a[0]) + 3.0 * (a[1] - a[2])) * (1.0 / 6.0)

    def sums_of(v):
        at = slice(v * 8, v * 8 + 8)
        knot = knot_v[at, :]
        u = phase_v[at, :]
        time = time_v[at, :]
        block = (sub + v * 8) * segs + lane // span
        chunk = (v * 8 * segs) // LANES
        count = lane_gather(count_v[chunk : chunk + 1, :], block - chunk * LANES)
        live = lane % span < count
        low, high = knot % LANES, knot // LANES
        picks = [high == c for c in range(n_chunks)]
        quat = []
        for m in range(4):
            value = None
            for j in (3, 2, 1, 0):
                got = lane_gather(coef[j, m : m + 1, :], low)
                for c in range(1, n_chunks):
                    x = c * 4 + m
                    got = jnp.where(picks[c], lane_gather(coef[j, x : x + 1, :], low), got)
                value = got if value is None else value * u + got
            quat.append(value)
        q0, q1, q2, q3 = quat
        cross = jnp.where(live, q0 * q0 + q1 * q1 - q2 * q2 - q3 * q3, 0.0)
        along = jnp.where(live, 2.0 * (q1 * q2 + q0 * q3), 0.0)
        tilt = 2.0 * (q1 * q3 - q0 * q2)
        parallax = jnp.where(live, parallax_v[at, :], 0.0)
        design = [cross, along, parallax, time * cross, time * along]
        residual = observed_v[at, :] - tilt
        return [design[i] * design[j] for i, j in PAIR_LIST] + [d * residual for d in design]

    for v in range(0, rows // 8, 2):
        first, second = sums_of(v), sums_of(v + 1)
        for x in range(20):
            for k, part in enumerate(split3(jnp.concatenate([first[x], second[x]], axis=0))):
                parts[k * rows + v * 8 : k * rows + v * 8 + 16, x * LANES : (x + 1) * LANES] = part

    three = jnp.dot(parts[...], spread[...], preferred_element_type=jnp.float32)
    block_sum = three[:rows] + three[rows : 2 * rows] + three[2 * rows :]
    stacked = jnp.concatenate(split3(block_sum), axis=0)
    by_seg = jnp.dot(member[...], stacked, preferred_element_type=jnp.float32)
    lane_s = lax.broadcasted_iota(jnp.int32, (sources, LANES), 1) // ROWS
    normal = jnp.where(lane_s == 0, by_seg[:sources], 0.0)
    for q in range(1, segs):
        normal = jnp.where(lane_s == q, by_seg[q * sources : (q + 1) * sources], normal)
    tiles[...] = normal.reshape(n_tm, owned, LANES)

    for d in range(1, n_tm):
        peer = lax.rem(tm + d, n_tm)
        pltpu.make_async_remote_copy(
            src_ref=tiles.at[peer],
            dst_ref=landed.at[d - 1],
            send_sem=sum_send,
            recv_sem=sum_recv,
            device_id={"tm": peer},
            device_id_type=MESH,
        ).start()
    total = tiles[tm]
    pltpu.make_async_copy(landed, landed, sum_recv).wait()
    for d in range(1, n_tm):
        total = total + landed[d - 1]
    out_ref[...] = total
    others = table.at[: n_sky - 1]
    pltpu.make_async_copy(others, others, att_send).wait()
    pltpu.make_async_copy(landed, landed, sum_send).wait()


def solve_kernel(total_ref, prior_hbm, out_ref, turned, prior_ref, sem):
    copy = pltpu.make_async_copy(prior_hbm, prior_ref, sem)
    copy.start()
    total = total_ref[...]
    full = total
    for shift in range(ROWS, LANES, ROWS):
        full = full + pltpu.roll(total, shift, 1)
    turned[...] = jnp.transpose(full)
    copy.wait()
    result = solve_rows(lambda i: turned[i : i + 1, :], lambda i: prior_ref[i : i + 1, :])
    for i in range(5):
        out_ref[i : i + 1, :] = result[i]


def on_device(n_sky, n_tm, attitude, time, parallax, observed, phase, knot, source, count, prior):
    slots, blocks, owned = time.shape[0], source.shape[0], prior.shape[1]
    knots = attitude.shape[2]
    rows = slots // LANES
    span = slots // blocks
    sources = owned * n_tm
    segs = LANES // span
    n_chunks = n_sky * knots // LANES
    shape = (rows, LANES)
    vmem = pltpu.VMEM
    f32, i32, bf16 = jnp.float32, jnp.int32, jnp.bfloat16
    total = pl.pallas_call(
        functools.partial(kernel, n_sky, n_tm, span),
        out_shape=pltpu.VMEM((owned, LANES), f32),
        in_specs=[pl.BlockSpec(memory_space=pl.ANY)] * 8,
        out_specs=pl.BlockSpec(memory_space=pltpu.VMEM),
        scratch_shapes=[
            vmem((n_sky, 4, knots), f32),
            vmem((4, n_chunks * 4, LANES), f32),
            vmem((4,) + shape, f32),
            vmem((rows + 2 * (blocks // LANES), LANES), i32),
            vmem((20 * LANES, LANES), bf16),
            vmem((3 * rows, 20 * LANES), bf16),
            vmem((segs * sources, 3 * rows), bf16),
            vmem((n_tm, owned, LANES), f32),
            vmem((n_tm - 1, owned, LANES), f32),
        ]
        + [pltpu.SemaphoreType.DMA] * 6,
        compiler_params=pltpu.CompilerParams(collective_id=0, has_side_effects=True),
    )(
        attitude.reshape(4, knots),
        time.reshape(shape),
        parallax.reshape(shape),
        observed.reshape(shape),
        phase.reshape(shape),
        knot.reshape(shape),
        source.reshape(blocks // LANES, LANES),
        count.reshape(blocks // LANES, LANES),
    )
    return pl.pallas_call(
        solve_kernel,
        out_shape=jax.ShapeDtypeStruct(prior.shape, f32),
        in_specs=[pl.BlockSpec(memory_space=pltpu.VMEM), pl.BlockSpec(memory_space=pl.ANY)],
        scratch_shapes=[vmem((LANES, owned), f32), vmem(prior.shape, f32), pltpu.SemaphoreType.DMA],
    )(pltpu.with_memory_space_constraint(total, pltpu.VMEM), prior)


def solution(mesh):
    slot = P(("sky", "tm"))
    in_specs = (P(None, "tm", "sky"),) + (slot,) * 7 + (P(None, ("sky", "tm")),)
    return jax.shard_map(
        functools.partial(on_device, mesh.shape["sky"], mesh.shape["tm"]),
        mesh=mesh,
        in_specs=in_specs,
        out_specs=P(None, ("sky", "tm")),
        check_vma=False,
    )
```

```python
import functools

import jax
import jax.numpy as jnp
from jax import lax
from jax.experimental import pallas as pl
from jax.experimental.pallas import tpu as pltpu
from jax.sharding import PartitionSpec as P

PAIR_LIST = [(i, j) for i in range(5) for j in range(i, 5)]
MESH = pl.DeviceIdType.MESH
LANES = 128
ROWS = 32


def lane_gather(row, index):
    wide = jnp.broadcast_to(row, index.shape)
    return jnp.take_along_axis(wide, index, axis=1, mode="promise_in_bounds")


def split3(value):
    high = value.astype(jnp.bfloat16)
    rest = value - high.astype(jnp.float32)
    mid = rest.astype(jnp.bfloat16)
    low = (rest - mid.astype(jnp.float32)).astype(jnp.bfloat16)
    return high, mid, low


def solve_rows(row, prior_row):
    entry = {}
    for index, (i, j) in enumerate(PAIR_LIST):
        entry[j, i] = row(index)
    for i in range(5):
        entry[i, i] = entry[i, i] + prior_row(i)
    right = [row(15 + i) for i in range(5)]
    unit, inverse = {}, []
    for col in range(5):
        inv = 1.0 / entry[col, col]
        inverse.append(inv)
        for r in range(col + 1, 5):
            unit[r, col] = entry[r, col] * inv
        for r in range(col + 1, 5):
            for c in range(col + 1, r + 1):
                entry[r, c] = entry[r, c] - unit[r, col] * entry[c, col]
            right[r] = right[r] - unit[r, col] * right[col]
    result = [right[i] * inverse[i] for i in range(5)]
    for i in range(4, 0, -1):
        for k in range(i):
            result[k] = result[k] - unit[i, k] * result[i]
    return result


def near_peers(tm, n_tm):
    if n_tm & (n_tm - 1):
        return [lax.rem(tm + d, n_tm) for d in range(1, n_tm)]
    bits = [1 << i for i in range(n_tm.bit_length() - 1)]
    return [tm + bit * (1 - 2 * ((tm // bit) % 2)) for bit in bits]


def meet(met, near, step):
    if step > 0:
        pl.semaphore_wait(met.at[step - 1], 1)
    if step < len(near) - 1:
        pl.semaphore_signal(
            met.at[step], inc=1, device_id={"tm": near[step + 1]}, device_id_type=MESH
        )


def kernel(
    n_sky, n_tm, span,
    attitude_hbm, time_hbm, parallax_hbm, observed_hbm, phase_hbm, knot_hbm,
    source_hbm, count_hbm, prior_hbm,
    out_ref, prior_ref,
    table, coef, reals, ints, spread, parts, member, tiles, landed,
    real_sem, int_sem, prior_sem, own_sem, att_send, att_recv, sum_send, sum_recv, met,
):
    sky = lax.axis_index("sky")
    tm = lax.axis_index("tm")
    rows = time_hbm.shape[0]
    owned = tiles.shape[1]
    wide = source_hbm.shape[0]
    phase_v, time_v, parallax_v, observed_v = (reals.at[i] for i in range(4))
    knot_v = ints.at[:rows]
    source_v = ints.at[rows : rows + wide]
    count_v = ints.at[rows + wide :]
    sources = owned * n_tm
    segs = LANES // span

    barrier = pltpu.get_barrier_semaphore()
    for d in range(1, n_sky):
        pl.semaphore_signal(
            barrier, inc=1, device_id={"sky": lax.rem(sky + d, n_sky)}, device_id_type=MESH
        )
    near = near_peers(tm, n_tm)
    for peer in near:
        pl.semaphore_signal(barrier, inc=1, device_id={"tm": peer}, device_id_type=MESH)
    own = pltpu.make_async_copy(attitude_hbm, table.at[sky], own_sem)
    own.start()
    for src, dst in ((source_hbm, source_v), (count_hbm, count_v), (knot_hbm, knot_v)):
        pltpu.make_async_copy(src, dst, int_sem).start()
    for i, src in enumerate((phase_hbm, time_hbm, parallax_hbm, observed_hbm)):
        pltpu.make_async_copy(src, reals.at[i], real_sem).start()
    prior_copy = pltpu.make_async_copy(prior_hbm, prior_ref, prior_sem)
    prior_copy.start()

    lane_out = lax.broadcasted_iota(jnp.int32, (LANES, LANES), 1)
    lane_in = lax.broadcasted_iota(jnp.int32, (LANES, LANES), 0)
    base = lane_out - (lane_in // span) * ROWS
    for x in range(20):
        spread[x * LANES : (x + 1) * LANES, :] = jnp.where(base == x, 1.0, 0.0).astype(jnp.bfloat16)

    own.wait()
    pl.semaphore_wait(barrier, n_sky - 1 + len(near))

    for d in range(1, n_sky):
        pltpu.make_async_remote_copy(
            src_ref=table.at[sky],
            dst_ref=table.at[sky],
            send_sem=att_send,
            recv_sem=att_recv,
            device_id={"sky": lax.rem(sky + d, n_sky)},
            device_id_type=MESH,
        ).start()

    meet(met, near, 0)
    pltpu.make_async_copy(ints, ints, int_sem).wait()

    width = 3 * rows
    lane = lax.broadcasted_iota(jnp.int32, (8, LANES), 1)
    sub = lax.broadcasted_iota(jnp.int32, (8, LANES), 0)
    id_list = []
    for start in range(0, width, LANES):
        block = ((lane + start) % rows) * segs + sub % segs
        got = lane_gather(source_v[0:1, :], block % LANES)
        for c in range(1, source_v.shape[0]):
            got = jnp.where(block // LANES == c, lane_gather(source_v[c : c + 1, :], block % LANES), got)
        id_list.append(got)
    ids = jnp.concatenate(id_list, axis=1)[:, :width]
    which = lax.broadcasted_iota(jnp.int32, (sources, width), 0)
    for q in range(segs):
        hit = jnp.broadcast_to(ids[q : q + 1, :], (sources, width)) == which
        member[q * sources : (q + 1) * sources, :] = jnp.where(hit, 1.0, 0.0).astype(jnp.bfloat16)

    for step in range(1, len(near) - 1):
        meet(met, near, step)
    pltpu.make_async_copy(reals, reals, real_sem).wait()
    others = table.at[: n_sky - 1]
    pltpu.make_async_copy(others, others, att_recv).wait()

    per = table.shape[2] // LANES
    chunks = [
        table[c // per, :, (c % per) * LANES : (c % per + 1) * LANES] for c in range(n_sky * per)
    ]
    n_chunks = len(chunks)
    here = jnp.concatenate(chunks, axis=0)
    after = jnp.concatenate(chunks[1:] + chunks[-1:], axis=0)
    wide_lane = lax.broadcasted_iota(jnp.int32, here.shape, 1)
    a = [here]
    for i in range(1, 4):
        a.append(
            jnp.where(
                wide_lane < LANES - i,
                pltpu.roll(here, LANES - i, 1),
                pltpu.roll(after, LANES - i, 1),
            )
        )
    coef[0] = (a[0] + 4.0 * a[1] + a[2]) * (1.0 / 6.0)
    coef[1] = (a[2] - a[0]) * 0.5
    coef[2] = (a[0] - 2.0 * a[1] + a[2]) * 0.5
    coef[3] = ((a[3] - a[0]) + 3.0 * (a[1] - a[2])) * (1.0 / 6.0)

    def sums_of(v):
        at = slice(v * 8, v * 8 + 8)
        knot = knot_v[at, :]
        u = phase_v[at, :]
        time = time_v[at, :]
        block = (sub + v * 8) * segs + lane // span
        chunk = (v * 8 * segs) // LANES
        count = lane_gather(count_v[chunk : chunk + 1, :], block - chunk * LANES)
        live = lane % span < count
        low, high = knot % LANES, knot // LANES
        picks = [high == c for c in range(n_chunks)]
        quat = []
        for m in range(4):
            value = None
            for j in (3, 2, 1, 0):
                got = lane_gather(coef[j, m : m + 1, :], low)
                for c in range(1, n_chunks):
                    x = c * 4 + m
                    got = jnp.where(picks[c], lane_gather(coef[j, x : x + 1, :], low), got)
                value = got if value is None else value * u + got
            quat.append(value)
        q0, q1, q2, q3 = quat
        cross = jnp.where(live, q0 * q0 + q1 * q1 - q2 * q2 - q3 * q3, 0.0)
        along = jnp.where(live, 2.0 * (q1 * q2 + q0 * q3), 0.0)
        tilt = 2.0 * (q1 * q3 - q0 * q2)
        parallax = jnp.where(live, parallax_v[at, :], 0.0)
        design = [cross, along, parallax, time * cross, time * along]
        residual = observed_v[at, :] - tilt
        return [design[i] * design[j] for i, j in PAIR_LIST] + [d * residual for d in design]

    for v in range(0, rows // 8, 2):
        first, second = sums_of(v), sums_of(v + 1)
        for x in range(20):
            for k, part in enumerate(split3(jnp.concatenate([first[x], second[x]], axis=0))):
                parts[k * rows + v * 8 : k * rows + v * 8 + 16, x * LANES : (x + 1) * LANES] = part

    three = jnp.dot(parts[...], spread[...], preferred_element_type=jnp.float32)
    block_sum = three[:rows] + three[rows : 2 * rows] + three[2 * rows :]
    stacked = jnp.concatenate(split3(block_sum), axis=0)
    by_seg = jnp.dot(member[...], stacked, preferred_element_type=jnp.float32)
    lane_s = lax.broadcasted_iota(jnp.int32, (sources, LANES), 1) // ROWS
    normal = jnp.where(lane_s == 0, by_seg[:sources], 0.0)
    for q in range(1, segs):
        normal = jnp.where(lane_s == q, by_seg[q * sources : (q + 1) * sources], normal)
    tiles[...] = normal.reshape(n_tm, owned, LANES)
    if len(near) > 1:
        pl.semaphore_wait(met.at[len(near) - 2], 1)

    for d in range(1, n_tm):
        peer = lax.rem(tm + d, n_tm)
        pltpu.make_async_remote_copy(
            src_ref=tiles.at[peer],
            dst_ref=landed.at[d - 1],
            send_sem=sum_send,
            recv_sem=sum_recv,
            device_id={"tm": peer},
            device_id_type=MESH,
        ).start()
    total = tiles[tm]
    pltpu.make_async_copy(landed, landed, sum_recv).wait()
    for d in range(1, n_tm):
        total = total + landed[d - 1]
    out_ref[...] = total
    prior_copy.wait()
    pltpu.make_async_copy(others, others, att_send).wait()
    pltpu.make_async_copy(landed, landed, sum_send).wait()


def solve_kernel(total_ref, prior_ref, out_ref, turned):
    total = total_ref[...]
    full = total
    for shift in range(ROWS, LANES, ROWS):
        full = full + pltpu.roll(total, shift, 1)
    turned[...] = jnp.transpose(full)
    result = solve_rows(lambda i: turned[i : i + 1, :], lambda i: prior_ref[i : i + 1, :])
    for i in range(5):
        out_ref[i : i + 1, :] = result[i]


def on_device(n_sky, n_tm, attitude, time, parallax, observed, phase, knot, source, count, prior):
    slots, blocks, owned = time.shape[0], source.shape[0], prior.shape[1]
    knots = attitude.shape[2]
    rows = slots // LANES
    span = slots // blocks
    sources = owned * n_tm
    segs = LANES // span
    n_chunks = n_sky * knots // LANES
    shape = (rows, LANES)
    vmem = pltpu.VMEM
    f32, i32, bf16 = jnp.float32, jnp.int32, jnp.bfloat16
    total, prior_near = pl.pallas_call(
        functools.partial(kernel, n_sky, n_tm, span),
        out_shape=(pltpu.VMEM((owned, LANES), f32), pltpu.VMEM(prior.shape, f32)),
        in_specs=[pl.BlockSpec(memory_space=pl.ANY)] * 9,
        out_specs=(pl.BlockSpec(memory_space=pltpu.VMEM),) * 2,
        scratch_shapes=[
            vmem((n_sky, 4, knots), f32),
            vmem((4, n_chunks * 4, LANES), f32),
            vmem((4,) + shape, f32),
            vmem((rows + 2 * (blocks // LANES), LANES), i32),
            vmem((20 * LANES, LANES), bf16),
            vmem((3 * rows, 20 * LANES), bf16),
            vmem((segs * sources, 3 * rows), bf16),
            vmem((n_tm, owned, LANES), f32),
            vmem((n_tm - 1, owned, LANES), f32),
        ]
        + [pltpu.SemaphoreType.DMA] * 8
        + [pltpu.SemaphoreType.REGULAR((max(1, len(near_peers(0, n_tm)) - 1),))],
        compiler_params=pltpu.CompilerParams(collective_id=0, has_side_effects=True),
    )(
        attitude.reshape(4, knots),
        time.reshape(shape),
        parallax.reshape(shape),
        observed.reshape(shape),
        phase.reshape(shape),
        knot.reshape(shape),
        source.reshape(blocks // LANES, LANES),
        count.reshape(blocks // LANES, LANES),
        prior,
    )
    return pl.pallas_call(
        solve_kernel,
        out_shape=jax.ShapeDtypeStruct(prior.shape, f32),
        in_specs=[pl.BlockSpec(memory_space=pltpu.VMEM)] * 2,
        scratch_shapes=[vmem((LANES, owned), f32)],
    )(
        pltpu.with_memory_space_constraint(total, pltpu.VMEM),
        pltpu.with_memory_space_constraint(prior_near, pltpu.VMEM),
    )


def solution(mesh):
    slot = P(("sky", "tm"))
    in_specs = (P(None, "tm", "sky"),) + (slot,) * 7 + (P(None, ("sky", "tm")),)
    return jax.shard_map(
        functools.partial(on_device, mesh.shape["sky"], mesh.shape["tm"]),
        mesh=mesh,
        in_specs=in_specs,
        out_specs=P(None, ("sky", "tm")),
        check_vma=False,
    )
```

```python
import functools

import jax
import jax.numpy as jnp
from jax import lax
from jax.experimental import pallas as pl
from jax.experimental.pallas import tpu as pltpu
from jax.sharding import PartitionSpec as P

PAIR_LIST = [(i, j) for i in range(5) for j in range(i, 5)]
MESH = pl.DeviceIdType.MESH
LANES = 128
ROWS = 32


def lane_gather(row, index):
    wide = jnp.broadcast_to(row, index.shape)
    return jnp.take_along_axis(wide, index, axis=1, mode="promise_in_bounds")


def split3(value):
    high = value.astype(jnp.bfloat16)
    rest = value - high.astype(jnp.float32)
    mid = rest.astype(jnp.bfloat16)
    low = (rest - mid.astype(jnp.float32)).astype(jnp.bfloat16)
    return high, mid, low


def split2(value):
    high = value.astype(jnp.bfloat16)
    return high, (value - high.astype(jnp.float32)).astype(jnp.bfloat16)


def solve_rows(row, prior_row):
    entry = {}
    for index, (i, j) in enumerate(PAIR_LIST):
        entry[j, i] = row(index)
    for i in range(5):
        entry[i, i] = entry[i, i] + prior_row(i)
    right = [row(15 + i) for i in range(5)]
    unit, inverse = {}, []
    for col in range(5):
        inv = 1.0 / entry[col, col]
        inverse.append(inv)
        for r in range(col + 1, 5):
            unit[r, col] = entry[r, col] * inv
        for r in range(col + 1, 5):
            for c in range(col + 1, r + 1):
                entry[r, c] = entry[r, c] - unit[r, col] * entry[c, col]
            right[r] = right[r] - unit[r, col] * right[col]
    result = [right[i] * inverse[i] for i in range(5)]
    for i in range(4, 0, -1):
        for k in range(i):
            result[k] = result[k] - unit[i, k] * result[i]
    return result


def near_peers(tm, n_tm):
    if n_tm % 2 == 0 and n_tm <= 8:
        edges = [(tm + 1 - 2 * (tm % 2), None), (tm + 2, tm + 2 < n_tm), (tm - 2, tm >= 2)]
        return edges, n_tm // 2 - 1
    if n_tm & (n_tm - 1) == 0:
        bits = [1 << i for i in range(n_tm.bit_length() - 1)]
        return [(tm + bit * (1 - 2 * ((tm // bit) % 2)), None) for bit in bits], len(bits) - 1
    return [(lax.rem(tm + d, n_tm), None) for d in range(1, n_tm)], 0


def tell(semaphore, edges):
    for peer, exists in edges:

        def send(peer=peer):
            pl.semaphore_signal(semaphore, inc=1, device_id={"tm": peer}, device_id_type=MESH)

        if exists is None:
            send()
        else:
            pl.when(exists)(send)


def kernel(
    n_sky, n_tm, span,
    attitude_hbm, time_hbm, parallax_hbm, observed_hbm, phase_hbm, knot_hbm,
    source_hbm, count_hbm, prior_hbm,
    out_ref, prior_ref,
    table, coef, reals, ints, spread, parts, member, tiles, landed,
    real_sem, int_sem, prior_sem, own_sem, att_send, att_recv, sum_send, sum_recv, met,
):
    sky = lax.axis_index("sky")
    tm = lax.axis_index("tm")
    rows = time_hbm.shape[0]
    owned = tiles.shape[1]
    wide = source_hbm.shape[0]
    phase_v, time_v, parallax_v, observed_v = (reals.at[i] for i in range(4))
    knot_v = ints.at[:rows]
    source_v = ints.at[rows : rows + wide]
    count_v = ints.at[rows + wide :]
    sources = owned * n_tm
    segs = LANES // span

    barrier = pltpu.get_barrier_semaphore()
    for d in range(1, n_sky):
        pl.semaphore_signal(
            barrier, inc=1, device_id={"sky": lax.rem(sky + d, n_sky)}, device_id_type=MESH
        )
    edges, rounds = near_peers(tm, n_tm)
    degree = sum(1 if exists is None else exists.astype(jnp.int32) for _, exists in edges)
    tell(barrier, edges)
    own = pltpu.make_async_copy(attitude_hbm, table.at[sky], own_sem)
    own.start()
    for src, dst in ((source_hbm, source_v), (count_hbm, count_v), (knot_hbm, knot_v)):
        pltpu.make_async_copy(src, dst, int_sem).start()
    for i, src in enumerate((phase_hbm, time_hbm, parallax_hbm, observed_hbm)):
        pltpu.make_async_copy(src, reals.at[i], real_sem).start()
    prior_copy = pltpu.make_async_copy(prior_hbm, prior_ref, prior_sem)
    prior_copy.start()

    lane_out = lax.broadcasted_iota(jnp.int32, (LANES, LANES), 1)
    lane_in = lax.broadcasted_iota(jnp.int32, (LANES, LANES), 0)
    base = lane_out - (lane_in // span) * ROWS
    for x in range(20):
        spread[x * LANES : (x + 1) * LANES, :] = jnp.where(base == x, 1.0, 0.0).astype(jnp.bfloat16)

    own.wait()
    pl.semaphore_wait(barrier, n_sky - 1 + degree)

    for d in range(1, n_sky):
        pltpu.make_async_remote_copy(
            src_ref=table.at[sky],
            dst_ref=table.at[sky],
            send_sem=att_send,
            recv_sem=att_recv,
            device_id={"sky": lax.rem(sky + d, n_sky)},
            device_id_type=MESH,
        ).start()

    if rounds:
        tell(met.at[0], edges)
    pltpu.make_async_copy(ints, ints, int_sem).wait()

    width = 3 * rows
    lane = lax.broadcasted_iota(jnp.int32, (8, LANES), 1)
    sub = lax.broadcasted_iota(jnp.int32, (8, LANES), 0)
    id_list = []
    for start in range(0, width, LANES):
        block = ((lane + start) % rows) * segs + sub % segs
        got = lane_gather(source_v[0:1, :], block % LANES)
        for c in range(1, source_v.shape[0]):
            got = jnp.where(block // LANES == c, lane_gather(source_v[c : c + 1, :], block % LANES), got)
        id_list.append(got)
    ids = jnp.concatenate(id_list, axis=1)[:, :width]
    which = lax.broadcasted_iota(jnp.int32, (sources, width), 0)
    for q in range(segs):
        hit = jnp.broadcast_to(ids[q : q + 1, :], (sources, width)) == which
        member[q * sources : (q + 1) * sources, :] = jnp.where(hit, 1.0, 0.0).astype(jnp.bfloat16)

    for step in range(1, min(2, rounds)):
        pl.semaphore_wait(met.at[step - 1], degree)
        tell(met.at[step], edges)
    pltpu.make_async_copy(reals, reals, real_sem).wait()
    others = table.at[: n_sky - 1]
    pltpu.make_async_copy(others, others, att_recv).wait()

    for step in range(2, rounds):
        pl.semaphore_wait(met.at[step - 1], degree)
        tell(met.at[step], edges)

    per = table.shape[2] // LANES
    chunks = [
        table[c // per, :, (c % per) * LANES : (c % per + 1) * LANES] for c in range(n_sky * per)
    ]
    n_chunks = len(chunks)
    here = jnp.concatenate(chunks, axis=0)
    after = jnp.concatenate(chunks[1:] + chunks[-1:], axis=0)
    wide_lane = lax.broadcasted_iota(jnp.int32, here.shape, 1)
    a = [here]
    for i in range(1, 4):
        a.append(
            jnp.where(
                wide_lane < LANES - i,
                pltpu.roll(here, LANES - i, 1),
                pltpu.roll(after, LANES - i, 1),
            )
        )
    coef[0] = (a[0] + 4.0 * a[1] + a[2]) * (1.0 / 6.0)
    coef[1] = (a[2] - a[0]) * 0.5
    coef[2] = (a[0] - 2.0 * a[1] + a[2]) * 0.5
    coef[3] = ((a[3] - a[0]) + 3.0 * (a[1] - a[2])) * (1.0 / 6.0)

    def sums_of(v):
        at = slice(v * 8, v * 8 + 8)
        knot = knot_v[at, :]
        u = phase_v[at, :]
        time = time_v[at, :]
        block = (sub + v * 8) * segs + lane // span
        chunk = (v * 8 * segs) // LANES
        count = lane_gather(count_v[chunk : chunk + 1, :], block - chunk * LANES)
        live = lane % span < count
        low, high = knot % LANES, knot // LANES
        picks = [high == c for c in range(n_chunks)]
        quat = []
        for m in range(4):
            value = None
            for j in (3, 2, 1, 0):
                got = lane_gather(coef[j, m : m + 1, :], low)
                for c in range(1, n_chunks):
                    x = c * 4 + m
                    got = jnp.where(picks[c], lane_gather(coef[j, x : x + 1, :], low), got)
                value = got if value is None else value * u + got
            quat.append(value)
        q0, q1, q2, q3 = quat
        cross = jnp.where(live, q0 * q0 + q1 * q1 - q2 * q2 - q3 * q3, 0.0)
        along = jnp.where(live, 2.0 * (q1 * q2 + q0 * q3), 0.0)
        tilt = 2.0 * (q1 * q3 - q0 * q2)
        parallax = jnp.where(live, parallax_v[at, :], 0.0)
        design = [cross, along, parallax, time * cross, time * along]
        residual = observed_v[at, :] - tilt
        return [design[i] * design[j] for i, j in PAIR_LIST] + [d * residual for d in design]

    for v in range(0, rows // 8, 2):
        first, second = sums_of(v), sums_of(v + 1)
        for x in range(20):
            for k, part in enumerate(split2(jnp.concatenate([first[x], second[x]], axis=0))):
                parts[k * rows + v * 8 : k * rows + v * 8 + 16, x * LANES : (x + 1) * LANES] = part

    two = jnp.dot(parts[...], spread[...], preferred_element_type=jnp.float32)
    block_sum = two[:rows] + two[rows:]
    stacked = jnp.concatenate(split3(block_sum), axis=0)
    by_seg = jnp.dot(member[...], stacked, preferred_element_type=jnp.float32)
    lane_s = lax.broadcasted_iota(jnp.int32, (sources, LANES), 1) // ROWS
    normal = jnp.where(lane_s == 0, by_seg[:sources], 0.0)
    for q in range(1, segs):
        normal = jnp.where(lane_s == q, by_seg[q * sources : (q + 1) * sources], normal)
    tiles[...] = normal.reshape(n_tm, owned, LANES)
    if rounds:
        pl.semaphore_wait(met.at[rounds - 1], degree)

    for d in range(1, n_tm):
        peer = lax.rem(tm + d, n_tm)
        pltpu.make_async_remote_copy(
            src_ref=tiles.at[peer],
            dst_ref=landed.at[d - 1],
            send_sem=sum_send,
            recv_sem=sum_recv,
            device_id={"tm": peer},
            device_id_type=MESH,
        ).start()
    total = tiles[tm]
    pltpu.make_async_copy(landed, landed, sum_recv).wait()
    for d in range(1, n_tm):
        total = total + landed[d - 1]
    out_ref[...] = total
    prior_copy.wait()
    pltpu.make_async_copy(others, others, att_send).wait()
    pltpu.make_async_copy(landed, landed, sum_send).wait()


def solve_kernel(total_ref, prior_ref, out_ref, turned):
    total = total_ref[...]
    full = total
    for shift in range(ROWS, LANES, ROWS):
        full = full + pltpu.roll(total, shift, 1)
    turned[...] = jnp.transpose(full)
    result = solve_rows(lambda i: turned[i : i + 1, :], lambda i: prior_ref[i : i + 1, :])
    for i in range(5):
        out_ref[i : i + 1, :] = result[i]


def on_device(n_sky, n_tm, attitude, time, parallax, observed, phase, knot, source, count, prior):
    slots, blocks, owned = time.shape[0], source.shape[0], prior.shape[1]
    knots = attitude.shape[2]
    rows = slots // LANES
    span = slots // blocks
    sources = owned * n_tm
    segs = LANES // span
    n_chunks = n_sky * knots // LANES
    shape = (rows, LANES)
    vmem = pltpu.VMEM
    f32, i32, bf16 = jnp.float32, jnp.int32, jnp.bfloat16
    total, prior_near = pl.pallas_call(
        functools.partial(kernel, n_sky, n_tm, span),
        out_shape=(pltpu.VMEM((owned, LANES), f32), pltpu.VMEM(prior.shape, f32)),
        in_specs=[pl.BlockSpec(memory_space=pl.ANY)] * 9,
        out_specs=(pl.BlockSpec(memory_space=pltpu.VMEM),) * 2,
        scratch_shapes=[
            vmem((n_sky, 4, knots), f32),
            vmem((4, n_chunks * 4, LANES), f32),
            vmem((4,) + shape, f32),
            vmem((rows + 2 * (blocks // LANES), LANES), i32),
            vmem((20 * LANES, LANES), bf16),
            vmem((2 * rows, 20 * LANES), bf16),
            vmem((segs * sources, 3 * rows), bf16),
            vmem((n_tm, owned, LANES), f32),
            vmem((n_tm - 1, owned, LANES), f32),
        ]
        + [pltpu.SemaphoreType.DMA] * 8
        + [pltpu.SemaphoreType.REGULAR((max(1, near_peers(0, n_tm)[1]),))],
        compiler_params=pltpu.CompilerParams(collective_id=0, has_side_effects=True),
    )(
        attitude.reshape(4, knots),
        time.reshape(shape),
        parallax.reshape(shape),
        observed.reshape(shape),
        phase.reshape(shape),
        knot.reshape(shape),
        source.reshape(blocks // LANES, LANES),
        count.reshape(blocks // LANES, LANES),
        prior,
    )
    return pl.pallas_call(
        solve_kernel,
        out_shape=jax.ShapeDtypeStruct(prior.shape, f32),
        in_specs=[pl.BlockSpec(memory_space=pltpu.VMEM)] * 2,
        scratch_shapes=[vmem((LANES, owned), f32)],
    )(
        pltpu.with_memory_space_constraint(total, pltpu.VMEM),
        pltpu.with_memory_space_constraint(prior_near, pltpu.VMEM),
    )


def solution(mesh):
    slot = P(("sky", "tm"))
    in_specs = (P(None, "tm", "sky"),) + (slot,) * 7 + (P(None, ("sky", "tm")),)
    return jax.shard_map(
        functools.partial(on_device, mesh.shape["sky"], mesh.shape["tm"]),
        mesh=mesh,
        in_specs=in_specs,
        out_specs=P(None, ("sky", "tm")),
        check_vma=False,
    )
```
